32 devices in a mesh: dp: 4 (over z), tensor: 8 (over y, x, core).
Axes of the slice: x: 2, y: 2, z: 4, core: 2. Of those that a mesh axis runs over, the one named last changes fastest.
Arguments:
- activations: bfloat16 [1024, 27648], P('dp', 'tensor'), may hold values from -6 to 6
- left_factor: float32 [216, 216], replicated, may hold values from -2 to 3, as said below
- right_factor: float32 [128, 128], replicated, may hold values from -2 to 3, as said below
- clip_scale: float32 [128, 216], replicated, may hold values from 0.5 to 3
- weight_rows: bfloat16 [27648, 5120], P('tensor'), may hold values from -0.0390625 to 0.0390625
- target: bfloat16 [1024, 5120], P('dp'), may hold values from -6 to 6
Outputs:
- grad_left: float32 [216, 216], replicated
- grad_right: float32 [128, 128], replicated
- grad_input: float32 [1024, 27648], P('dp', 'tensor')
The draws below stay inside these ranges and needn't reach their ends.
Inputs may be any that keep to these rules, and one draw needn't show every extreme that they name: `left_factor`: the identity plus independent entries of order one over the square root of 216. `right_factor`: the identity plus independent entries of order one over the square root of 128.
All inputs are finite; a program needn't handle non-finite values.
Results may differ from the reference program's by a relative error of at most 0.007.
Values may be sent and summed in bfloat16 or wider, within the bound.
A program may use at most 128 MiB of HBM per device.

```python
import math
import jax
import jax.numpy as jnp
from jax import lax

OUT = 5120
F1 = 216
F2 = 128
HID = 27648
TOKENS = 1024


def make_factor(key, order):
    noise = jnp.clip(jax.random.normal(key, (order, order), jnp.float32), -4.0, 4.0)
    return jnp.eye(order, dtype=jnp.float32) + noise / jnp.sqrt(order * 1.0)


def draw_left_factor(key, part):
    return make_factor(jax.random.fold_in(key, 11), F1)


def draw_right_factor(key, part):
    return make_factor(jax.random.fold_in(key, 23), F2)


def block_levels(key, shape, pieces, low, high):
    def one(dim, blocks):
        steps = jax.random.uniform(jax.random.fold_in(jax.random.fold_in(key, 6), dim), (blocks,), jnp.float32, low / len(pieces), high / len(pieces))
        return jnp.repeat(jnp.exp(steps), shape[dim] // blocks).reshape((-1,) + (1,) * (len(shape) - dim - 1))

    factor_of = one(*pieces[0])
    for cut in pieces[1:]:
        factor_of = factor_of * one(*cut)
    return factor_of


def normal_values(stream_key, shape, spread, bound, pieces=(), kind=jnp.bfloat16):
    loudness = block_levels(stream_key, shape, pieces, -0.22, 0.18) if pieces else 1.0
    values = jax.random.normal(stream_key, shape, jnp.float32) * spread * loudness
    return jnp.minimum(jnp.maximum(values, -bound), bound).astype(kind)


def setup_inputs(seed: int = 0) -> dict:
    seeds = jax.random.split(jax.random.key(seed), 7)
    activations = normal_values(seeds[0], (TOKENS, HID), 1.0, 6.0, ((0, 4), (1, 8)))
    left_factor = draw_left_factor(jax.random.fold_in(seeds[6], 71), 0)
    right_factor = draw_right_factor(jax.random.fold_in(seeds[6], 71), 0)
    clip_scale = jnp.clip(jnp.exp(jax.random.uniform(seeds[3], (F2, F1), jnp.float32, math.log(0.5), math.log(3.0))), 0.5, 3.0)
    weight_rows = normal_values(seeds[4], (HID, OUT), HID ** -0.5, 0.0390625, ((0, 8),))
    target = normal_values(seeds[5], (TOKENS, OUT), 1.0, 6.0, ((0, 4),))
    return dict(activations=activations, left_factor=left_factor, right_factor=right_factor, clip_scale=clip_scale, weight_rows=weight_rows, target=target)


def reference(activations, left_factor, right_factor, clip_scale, weight_rows, target):
    highest = lax.Precision.HIGHEST
    inputs = activations.reshape(TOKENS, F2, F1).astype(jnp.float32)
    mixed = jnp.einsum('tji,ik->tjk', inputs, left_factor, precision=highest)
    rotated = jnp.einsum('jl,tjk->tlk', right_factor, mixed, precision=highest)
    bounded = jnp.tanh(rotated / clip_scale)
    clipped = (clip_scale * bounded).astype(jnp.bfloat16).reshape(TOKENS, HID)
    output = jnp.dot(clipped, weight_rows, preferred_element_type=jnp.float32)
    out_grad = (output - target.astype(jnp.float32)).astype(jnp.bfloat16)
    clipped_grad = lax.dot_general(out_grad, weight_rows, (((1,), (1,)), ((), ())), preferred_element_type=jnp.float32)
    rotated_grad = clipped_grad.reshape(TOKENS, F2, F1) * (1.0 - bounded * bounded)
    mixed_grad = jnp.einsum('jl,tlk->tjk', right_factor, rotated_grad, precision=highest)
    grad_right = jnp.einsum('tjk,tlk->jl', mixed, rotated_grad, precision=highest)
    grad_left = jnp.einsum('tji,tjk->ik', inputs, mixed_grad, precision=highest)
    grad_input = jnp.einsum('tjk,ik->tji', mixed_grad, left_factor, precision=highest).reshape(TOKENS, HID)
    return grad_left, grad_right, grad_input
```

```python
import jax
import jax.numpy as jnp
from jax import lax
from jax.experimental import pallas as pl
from jax.experimental.pallas import tpu as pltpu
from jax.sharding import PartitionSpec as P

BF = jnp.bfloat16
F32 = jnp.float32


def finish_kernel(grad_ref, act_ref, factor_ref, out_ref, left_ref):
    order = factor_ref.shape[0]
    factor = factor_ref[...]

    @pl.when(pl.program_id(0) == 0)
    def _():
        left_ref[...] = jnp.zeros_like(left_ref)

    total = jnp.zeros((order, order), F32)
    for j in range(grad_ref.shape[1] // order):
        here = slice(j * order, (j + 1) * order)
        grad = grad_ref[:, here]
        out_ref[:, here] = lax.dot_general(
            grad, factor, (((1,), (1,)), ((), ())), preferred_element_type=F32
        )
        total = total + lax.dot_general(
            act_ref[:, here], grad, (((0,), (0,)), ((), ())), preferred_element_type=F32
        )
    left_ref[...] += total


def finish(grad, act, factor):
    rows, width = grad.shape
    order = factor.shape[0]
    tile = min(rows, 128)
    return pl.pallas_call(
        finish_kernel,
        grid=(rows // tile,),
        in_specs=[
            pl.BlockSpec((tile, width), lambda i: (i, 0)),
            pl.BlockSpec((tile, width), lambda i: (i, 0)),
            pl.BlockSpec((order, order), lambda i: (0, 0)),
        ],
        out_specs=[
            pl.BlockSpec((tile, width), lambda i: (i, 0)),
            pl.BlockSpec((order, order), lambda i: (0, 0)),
        ],
        out_shape=[
            jax.ShapeDtypeStruct((rows, width), F32),
            jax.ShapeDtypeStruct((order, order), F32),
        ],
        compiler_params=pltpu.CompilerParams(vmem_limit_bytes=48 * 1024 * 1024),
        cost_estimate=pl.CostEstimate(
            flops=4 * rows * width * order, bytes_accessed=8 * rows * width, transcendentals=0
        ),
    )(grad, act, factor.astype(BF))


def split(value):
    head = value.astype(BF)
    return head, (value - head.astype(F32)).astype(BF)


def dot(a, b, dims):
    return lax.dot_general(a, b, ((dims[:1], dims[1:]), ((), ())), preferred_element_type=F32)


def forward_kernel(
    act_ref, left_ref, right_ref, clip_ref, out_ref, mixed_ref, bounded_ref, rows_ref, cols_ref
):
    peers, own, width = act_ref.shape
    order = left_ref.shape[0]
    each = width // order
    left_hi, left_lo = split(left_ref[...])
    right_hi, right_lo = split(right_ref[...])
    clip = clip_ref[...]

    @pl.loop(0, peers)
    def _(s):
        x = jnp.concatenate(
            [act_ref[s, :, j * order : (j + 1) * order] for j in range(each)], axis=0
        )
        mixed = dot(x, left_hi, (1, 0)) + dot(x, left_lo, (1, 0))
        for j in range(each):
            rows_ref[s * each + j] = mixed[j * own : (j + 1) * own]

    @pl.loop(0, own, unroll=4)
    def _(t):
        mixed = rows_ref[:, t, :]
        hi, lo = split(mixed)
        mixed_ref[t] = hi
        rotated = (
            dot(right_hi, hi, (0, 0)) + dot(right_lo, hi, (0, 0)) + dot(right_hi, lo, (0, 0))
        )
        bounded = jnp.tanh(rotated / clip)
        bounded_ref[t] = bounded
        cols_ref[:, t, :] = clip * bounded

    @pl.loop(0, peers)
    def _(s):
        for j in range(each):
            out_ref[s, :, j * order : (j + 1) * order] = cols_ref[s * each + j].astype(BF)


def backward_kernel(
    grad_ref, mixed_ref, bounded_ref, right_ref, out_ref, sum_ref, rows_ref, cols_ref
):
    peers, own, width = grad_ref.shape
    order = bounded_ref.shape[2]
    each = width // order
    right = right_ref[...].astype(BF)

    @pl.loop(0, peers)
    def _(s):
        for j in range(each):
            rows_ref[s * each + j] = grad_ref[s, :, j * order : (j + 1) * order].astype(F32)

    sum_ref[...] = jnp.zeros_like(sum_ref)

    @pl.loop(0, own, unroll=4)
    def _(t):
        bounded = bounded_ref[t]
        rotated_grad = (rows_ref[:, t, :] * (1.0 - bounded * bounded)).astype(BF)
        sum_ref[...] += dot(mixed_ref[t], rotated_grad, (1, 1))
        cols_ref[:, t, :] = dot(right, rotated_grad, (1, 0))

    @pl.loop(0, peers)
    def _(s):
        for j in range(each):
            out_ref[s, :, j * order : (j + 1) * order] = cols_ref[s * each + j].astype(BF)


def owner_call(kernel, outs, scratch, *args):
    return pl.pallas_call(
        kernel,
        out_shape=[jax.ShapeDtypeStruct(*out) for out in outs],
        in_specs=[pl.BlockSpec(memory_space=pltpu.VMEM)] * len(args),
        out_specs=[pl.BlockSpec(memory_space=pltpu.VMEM)] * len(outs),
        scratch_shapes=[pltpu.VMEM(scratch, F32)] * 2,
        compiler_params=pltpu.CompilerParams(vmem_limit_bytes=56 * 1024 * 1024),
    )(*args)


def local(activations, left_factor, right_factor, clip_scale, weight_rows, target):
    peers = lax.axis_size("tensor")
    everyone = lax.axis_size("dp") * peers
    tok_rows, width = activations.shape
    width_left = left_factor.shape[0]
    width_right = right_factor.shape[0]
    own = tok_rows // peers

    def exchange(blocks):
        got = lax.all_to_all(
            blocks.reshape(tok_rows, width), "tensor", split_axis=0, concat_axis=0, tiled=True
        )
        return got.reshape(peers, own, width)

    flat = (peers, own, width)
    cube = (own, width_right, width_left)
    by_row = (width_right, own, width_left)
    clipped, mixed, bounded = owner_call(
        forward_kernel, [(flat, BF), (cube, BF), (cube, F32)], by_row,
        exchange(activations), left_factor, right_factor, clip_scale,
    )
    clipped = exchange(clipped).reshape(tok_rows, width)
    partial_out = jnp.dot(clipped, weight_rows, preferred_element_type=F32).astype(BF)
    chips = peers // 2
    core = lax.axis_index("tensor") % 2
    same_core = [[2 * q + c for q in range(chips)] for c in range(2)]
    swap = [(d, d ^ 1) for d in range(peers)]
    blocks = partial_out.reshape(chips, 2, own, -1)
    there = lax.dynamic_index_in_dim(blocks, 1 - core, 1, keepdims=False)
    here = lax.dynamic_index_in_dim(blocks, core, 1, keepdims=False)
    there = lax.ppermute(there, "tensor", swap)
    paired = (here.astype(F32) + there.astype(F32)).astype(BF)
    terms = lax.all_to_all(
        paired, "tensor", split_axis=0, concat_axis=0, axis_index_groups=same_core, tiled=True
    )
    total = jnp.sum(terms.astype(F32), axis=0)
    mine = lax.dynamic_slice_in_dim(target, lax.axis_index("tensor") * own, own, 0)
    mine = (total - mine.astype(F32)).astype(BF)
    got = lax.all_to_all(
        jnp.broadcast_to(mine[None], (chips, *mine.shape)),
        "tensor", split_axis=0, concat_axis=0, axis_index_groups=same_core, tiled=True,
    )
    other = lax.ppermute(got, "tensor", swap)
    first = jnp.where(core == 0, got, other)
    second = jnp.where(core == 0, other, got)
    out_grad = jnp.stack([first, second], axis=1).reshape(tok_rows, -1)
    clipped_grad = lax.dot_general(
        out_grad, weight_rows, (((1,), (1,)), ((), ())), preferred_element_type=F32
    ).astype(BF)
    mixed_grad, right_part = owner_call(
        backward_kernel, [(flat, BF), ((width_right, width_right), F32)], by_row,
        exchange(clipped_grad), mixed, bounded, right_factor,
    )
    grad_back = exchange(mixed_grad).reshape(tok_rows, width)
    input_grad, left_part = finish(grad_back, activations, left_factor)

    cols = max(width_left, width_right)
    stacked = jnp.concatenate(
        [
            jnp.pad(left_part, ((0, 0), (0, cols - width_left))),
            jnp.pad(right_part, ((0, 0), (0, cols - width_right))),
        ],
        axis=0,
    )
    rows = -(-stacked.shape[0] // (8 * peers)) * 8
    stacked = jnp.pad(stacked, ((0, rows * peers - stacked.shape[0]), (0, 0)))

    def spread(piece, axis, times):
        copies = jnp.broadcast_to(piece[None], (times, *piece.shape))
        return lax.all_to_all(copies, axis, split_axis=0, concat_axis=0, tiled=True)

    shares = lax.all_to_all(
        stacked.reshape(peers, rows, cols), "tensor", split_axis=0, concat_axis=0, tiled=True
    )
    share = jnp.sum(spread(jnp.sum(shares, axis=0), "dp", lax.axis_size("dp")), axis=0)
    sums = spread(share, "tensor", peers).reshape(rows * peers, cols)
    left_sum = sums[:width_left, :width_left]
    right_sum = sums[width_left : width_left + width_right, :width_right]
    return (left_sum, right_sum, input_grad)


def solution(mesh):
    placed = (P("dp", "tensor"), P(), P(), P(), P("tensor", None), P("dp", None))
    return jax.shard_map(
        local, mesh=mesh, in_specs=placed, out_specs=(P(), P(), P("dp", "tensor")), check_vma=False
    )
```
